128 devices in a mesh: row: 8 (over z, y_lo), col: 16 (over x, y_hi, core).
Axes of the slice: x: 4, y: 4 (y_hi: 2, y_lo: 2; y = y_hi * 2 + y_lo), z: 4, core: 2. Of those that a mesh axis runs over, the one named last changes fastest.
Arguments:
- slab_pair: float32 [65536, 4096], P('row', 'col'), may hold values from -6 to 6, as said below
- butterfly_scale: float32 [65536], P('row'), may hold values from 0.5 to 2
Outputs:
- transformed: float32 [65536, 4096], P('row', 'col')
The draws below stay inside these ranges and needn't reach their ends.
Inputs may be any that keep to these rules, and one draw needn't show every extreme that they name: The matrix is symmetric where the slab pair meets its own columns: with g(k) = k for k < 2048 and 32768 + k - 2048 otherwise, slab_pair[g(a), b] = slab_pair[g(b), a] for all a, b below 4096.
All inputs are finite; a program needn't handle non-finite values.
Results may differ from the reference program's by a relative error of at most 0.00002.
Values sent between devices are 32-bit elements; how exact they have to be, the bound alone decides.
No kernel may reach another device: no remote copies, remote signals or barrier semaphores. Data moves between devices by JAX's collectives and lax.ppermute only.
A program may use at most 64 MiB of HBM per device.

```python
import math
import jax
import jax.numpy as jnp

N = 65536
W = 2048
HALF = 32768


def draw_slab_pair(key, part):
    base = jnp.clip(jax.random.normal(key, (N, 2 * W), jnp.float32), -6.0, 6.0)
    block = jnp.concatenate([base[:W], base[HALF:HALF + W]], axis=0)
    mirrored = jnp.clip((block + block.T) * jnp.float32(0.5) ** 0.5, -6.0, 6.0)
    base = base.at[:W].set(mirrored[:W])
    base = base.at[HALF:HALF + W].set(mirrored[W:])
    return base


def shard_levels(key, dims, pieces, smallest, largest):
    def one(axis_at, parts):
        steps = jax.random.uniform(jax.random.fold_in(jax.random.fold_in(key, 6), axis_at), (parts,), jnp.float32, smallest / len(pieces), largest / len(pieces))
        return jnp.repeat(jnp.exp(steps), dims[axis_at] // parts).reshape((-1,) + (1,) * (len(dims) - axis_at - 1))

    factor_of = one(*pieces[0])
    for cut in pieces[1:]:
        factor_of = factor_of * one(*cut)
    return factor_of


def setup_inputs(seed: int = 0) -> dict:
    arg_keys = jax.random.split(jax.random.key(seed), 3)
    slab_pair = draw_slab_pair(jax.random.fold_in(arg_keys[2], 71), 0)
    butterfly_scale = jnp.clip(jnp.exp(math.log(2.0) - 1.3862944 * jax.random.uniform(arg_keys[1], (N,), jnp.float32) ** shard_levels(arg_keys[1], (N,), ((0, 8),), -0.2, 0.2)), 0.5, 2.0)
    return dict(slab_pair=slab_pair, butterfly_scale=butterfly_scale)


def reference(slab_pair, butterfly_scale):
    root_two = jnp.float32(2.0) ** 0.5
    upper = slab_pair[:HALF]
    lower = slab_pair[HALF:]
    rows_top = butterfly_scale[:HALF, None] * (upper + lower) / root_two
    rows_bottom = butterfly_scale[HALF:, None] * (upper - lower) / root_two
    rows_mixed = jnp.concatenate([rows_top, rows_bottom], axis=0)
    column_scale = jnp.concatenate([butterfly_scale[:W], butterfly_scale[HALF:HALF + W]])
    left_part = rows_mixed[:, :W]
    right_part = rows_mixed[:, W:]
    both_mixed = jnp.concatenate([left_part + right_part, left_part - right_part], axis=1)
    both_mixed = both_mixed * column_scale[None, :] / root_two
    row_index = jnp.arange(N, dtype=jnp.int32)[:, None]
    col_index = jnp.arange(2 * W, dtype=jnp.int32)[None, :]
    global_col = jnp.where(col_index < W, col_index, HALF + col_index - W)
    return jnp.where(row_index >= global_col, both_mixed, jnp.float32(0.0))
```

```python
import math

import jax
import jax.numpy as jnp
from jax import lax
from jax.experimental import pallas as pl
from jax.sharding import PartitionSpec as P


N = 65536
W = 2048
LANES = 128
SIZES = (512, 2560, 768, 256)


def from_partner(block, axis):
    count = lax.axis_size(axis)
    return lax.ppermute(block, axis, [(i, i ^ count // 2) for i in range(count)])


def in_first_half(axis):
    return lax.axis_index(axis) < lax.axis_size(axis) // 2


def rows_spec(tile, cols, start):
    return pl.BlockSpec((tile, cols), lambda i: (start // tile + i, 0))


def copy_rows(x, start, size):
    tile = math.gcd(start, size)
    cols = x.shape[1]

    def kernel(x_ref, out_ref):
        out_ref[...] = x_ref[...]

    return pl.pallas_call(
        kernel,
        grid=(size // tile,),
        in_specs=[rows_spec(tile, cols, start)],
        out_specs=rows_spec(tile, cols, 0),
        out_shape=jax.ShapeDtypeStruct((size, cols), x.dtype),
    )(x)


def mix_rows(x, partner, start, axis):
    size, cols = partner.shape
    tile = math.gcd(start, size)

    def kernel(x_ref, partner_ref, out_ref):
        sign = jnp.where(in_first_half(axis), jnp.float32(1.0), jnp.float32(-1.0))
        out_ref[...] = partner_ref[...] + sign * x_ref[...]

    return pl.pallas_call(
        kernel,
        grid=(size // tile,),
        in_specs=[rows_spec(tile, cols, start), rows_spec(tile, cols, 0)],
        out_specs=rows_spec(tile, cols, 0),
        out_shape=jax.ShapeDtypeStruct((size, cols), x.dtype),
    )(x, partner)


def finish_rows(out, mixed, across, row_scale, col_scale, start, axis, local_rows):
    size, cols = mixed.shape
    tile = math.gcd(start, size)

    def kernel(mixed_ref, across_ref, row_scale_ref, col_scale_ref, *rest):
        out_ref = rest[-1]
        sign = jnp.where(in_first_half(axis), jnp.float32(1.0), jnp.float32(-1.0))
        first_row = lax.axis_index("row") * local_rows + start + pl.program_id(0) * tile
        first_col = lax.axis_index("col") * cols
        first_col = jnp.where(first_col < W, first_col, N // 2 + first_col - W)
        col_scales = col_scale_ref[...]
        lead = lax.broadcasted_iota(jnp.int32, (LANES, cols), 0) - lax.broadcasted_iota(
            jnp.int32, (LANES, cols), 1
        )
        for g in range(tile // LANES):
            rows = pl.ds(g * LANES, LANES)
            at = start // LANES + pl.program_id(0) * (tile // LANES) + g
            scale = jnp.broadcast_to(row_scale_ref[pl.ds(at, 1), :], (LANES, LANES)).T
            both = across_ref[rows, :] + sign * mixed_ref[rows, :]
            both = both * (jnp.concatenate([scale] * (cols // LANES), axis=1) * col_scales)
            keep = lead >= first_col - first_row - g * LANES
            out_ref[rows, :] = jnp.where(keep, both, jnp.float32(0.0))

    in_specs = [
        rows_spec(tile, cols, 0),
        rows_spec(tile, cols, 0),
        pl.BlockSpec(row_scale.shape, lambda i: (0, 0)),
        pl.BlockSpec(col_scale.shape, lambda i: (0, 0)),
    ]
    operands = [mixed, across, row_scale, col_scale]
    aliases = {}
    if out is not None:
        in_specs.append(pl.BlockSpec(memory_space=pl.ANY))
        operands.append(out)
        aliases = {4: 0}
    return pl.pallas_call(
        kernel,
        grid=(size // tile,),
        in_specs=in_specs,
        out_specs=rows_spec(tile, cols, start),
        out_shape=jax.ShapeDtypeStruct((local_rows, cols), mixed.dtype),
        input_output_aliases=aliases,
    )(*operands)


def per_device(slab_pair, butterfly_scale):
    local_rows, local_cols = slab_pair.shape
    row_count = lax.axis_size("row")
    parts = []
    start = 0
    for size in SIZES:
        parts.append((start, size, "row", "col"))
        parts.append((local_rows // 2 + start, size, "col", "row"))
        start += size

    theirs = []
    for start, size, first, _ in parts:
        block = copy_rows(slab_pair, start, size)
        theirs.append(from_partner(block, first))

    at = lax.axis_index("col") * local_cols % W
    piece = lax.dynamic_slice_in_dim(butterfly_scale, at, local_cols, 0)
    pieces = lax.all_gather(piece, "row", axis=0)
    left = in_first_half("col")
    col_scale = jnp.where(left, pieces[0], pieces[row_count // 2])[None, :] * 0.5
    row_scale = butterfly_scale.reshape(-1, LANES)

    mixes, acrosses = [], []
    for j, (start, size, first, second) in enumerate(parts):
        mixes.append(mix_rows(slab_pair, theirs[j], start, first))
        acrosses.append(from_partner(mixes[j], second))

    out = None
    for j, (start, size, first, second) in enumerate(parts):
        out = finish_rows(
            out, mixes[j], acrosses[j], row_scale, col_scale, start, second, local_rows
        )
    return out


def solution(mesh):
    in_specs = (P("row", "col"), P("row"))
    out_specs = P("row", "col")
    return jax.shard_map(
        per_device, mesh=mesh, in_specs=in_specs, out_specs=out_specs, check_vma=False
    )
```

```python
import jax
import jax.numpy as jnp
from jax import lax
from jax.experimental import pallas as pl
from jax.experimental.pallas import tpu as pltpu
from jax.sharding import PartitionSpec as P


N = 65536
W = 2048
SIZES = (512, 2688, 768, 128)


def from_partner(block, axis):
    count = lax.axis_size(axis)
    return lax.ppermute(block, axis, [(i, i ^ count // 2) for i in range(count)])


def in_first_half(axis):
    return lax.axis_index(axis) < lax.axis_size(axis) // 2


def kept_apart(*arrays):
    return lax.optimization_barrier(arrays)


def copy_rows(x, start, size):
    (x,) = kept_apart(x)
    return lax.slice_in_dim(x, start, start + size)


def mix_rows(x, partner, start, axis):
    x, partner = kept_apart(x, partner)
    block = lax.slice_in_dim(x, start, start + partner.shape[0])
    return jnp.where(in_first_half(axis), partner + block, partner - block)


def first_global_col(cols):
    first = lax.axis_index("col") * cols
    return jnp.where(first < W, first, N // 2 + first - W)


def unwritten(shape, dtype):
    return pl.pallas_call(
        lambda out_ref: None,
        out_specs=pl.BlockSpec(memory_space=pltpu.HBM),
        out_shape=jax.ShapeDtypeStruct(shape, dtype),
    )()


def finish_rows(out, mixed, across, row_scale, col_scale, start, axis):
    size, cols = mixed.shape
    both = jnp.where(in_first_half(axis), across + mixed, across - mixed)
    both = both * (row_scale[start : start + size, None] * col_scale)
    gap = first_global_col(cols) - lax.axis_index("row") * row_scale.shape[0] - start
    row = lax.broadcasted_iota(jnp.int32, (size, cols), 0)
    col = lax.broadcasted_iota(jnp.int32, (size, cols), 1)
    kept = jnp.where(row - col >= gap, both, jnp.float32(0.0))
    return lax.dynamic_update_slice(out, kept, (start, 0))


def per_device(slab_pair, butterfly_scale):
    local_rows, local_cols = slab_pair.shape
    row_count = lax.axis_size("row")
    parts = []
    start = 0
    for size in SIZES:
        parts.append((start, size, "row", "col"))
        parts.append((local_rows // 2 + start, size, "col", "row"))
        start += size

    theirs = []
    for start, size, first, _ in parts:
        block = copy_rows(slab_pair, start, size)
        theirs.append(from_partner(block, first))

    at = lax.axis_index("col") * local_cols % W
    piece = lax.dynamic_slice_in_dim(butterfly_scale, at, local_cols, 0)
    pieces = lax.all_gather(piece, "row", axis=0)
    left = in_first_half("col")
    col_scale = jnp.where(left, pieces[0], pieces[row_count // 2]) * 0.5

    mixes, acrosses = [], []
    for j, (start, size, first, second) in enumerate(parts):
        mixes.append(mix_rows(slab_pair, theirs[j], start, first))
        acrosses.append(from_partner(mixes[j], second))

    out = unwritten(slab_pair.shape, slab_pair.dtype)
    for j, (start, _, _, axis) in enumerate(parts):
        out = finish_rows(out, mixes[j], acrosses[j], butterfly_scale, col_scale, start, axis)
    return out


def solution(mesh):
    in_specs = (P("row", "col"), P("row"))
    out_specs = P("row", "col")
    return jax.shard_map(
        per_device, mesh=mesh, in_specs=in_specs, out_specs=out_specs, check_vma=False
    )
```

```python
import jax
import jax.numpy as jnp
from jax import lax
from jax.experimental import pallas as pl
from jax.experimental.pallas import tpu as pltpu
from jax.sharding import PartitionSpec as P


N = 65536
W = 2048
SIZES = (512, 2688, 704, 192)


def from_partner(block, axis):
    count = lax.axis_size(axis)
    return lax.ppermute(block, axis, [(i, i ^ count // 2) for i in range(count)])


def in_first_half(axis):
    return lax.axis_index(axis) < lax.axis_size(axis) // 2


def kept_apart(*arrays):
    return lax.optimization_barrier(arrays)


def copy_rows(x, start, size):
    (x,) = kept_apart(x)
    return lax.slice_in_dim(x, start, start + size)


def copy_first(x, starts, size):
    pieces = 4
    step = size // pieces

    def kernel(x_ref, *refs):
        out_refs, sems = refs[:-1], refs[-1]
        copies = []
        for p in range(pieces):
            for k, (start, out_ref) in enumerate(zip(starts, out_refs)):
                copies.append(
                    pltpu.make_async_copy(
                        x_ref.at[pl.ds(start + p * step, step), :],
                        out_ref.at[pl.ds(p * step, step), :],
                        sems.at[k, p],
                    )
                )
        for copy in copies:
            copy.start()
        for copy in copies:
            copy.wait()

    hbm = pl.BlockSpec(memory_space=pltpu.HBM)
    return pl.pallas_call(
        kernel,
        in_specs=[hbm],
        out_specs=[hbm] * len(starts),
        out_shape=[jax.ShapeDtypeStruct((size, x.shape[1]), x.dtype)] * len(starts),
        scratch_shapes=[pltpu.SemaphoreType.DMA((len(starts), pieces))],
    )(x)


def mix_rows(x, partner, start, axis):
    x, partner = kept_apart(x, partner)
    block = lax.slice_in_dim(x, start, start + partner.shape[0])
    return jnp.where(in_first_half(axis), partner + block, partner - block)


def first_global_col(cols):
    first = lax.axis_index("col") * cols
    return jnp.where(first < W, first, N // 2 + first - W)


def unwritten(shape, dtype):
    return pl.pallas_call(
        lambda out_ref: None,
        out_specs=pl.BlockSpec(memory_space=pltpu.HBM),
        out_shape=jax.ShapeDtypeStruct(shape, dtype),
    )()


def finish_rows(out, mixed, across, row_scale, col_scale, start, axis):
    size, cols = mixed.shape
    both = jnp.where(in_first_half(axis), across + mixed, across - mixed)
    both = both * (row_scale[start : start + size, None] * col_scale)
    gap = first_global_col(cols) - lax.axis_index("row") * row_scale.shape[0] - start
    row = lax.broadcasted_iota(jnp.int32, (size, cols), 0)
    col = lax.broadcasted_iota(jnp.int32, (size, cols), 1)
    kept = jnp.where(row - col >= gap, both, jnp.float32(0.0))
    return lax.dynamic_update_slice(out, kept, (start, 0))


def per_device(slab_pair, butterfly_scale):
    local_rows, local_cols = slab_pair.shape
    row_count = lax.axis_size("row")
    parts = []
    start = 0
    for size in SIZES:
        parts.append((start, size, "row", "col"))
        parts.append((local_rows // 2 + start, size, "col", "row"))
        start += size

    theirs = []
    firsts = copy_first(slab_pair, [part[0] for part in parts[:2]], SIZES[0])
    for j, (start, size, first, _) in enumerate(parts):
        block = firsts[j] if j < 2 else copy_rows(slab_pair, start, size)
        theirs.append(from_partner(block, first))

    at = lax.axis_index("col") * local_cols % W
    piece = lax.dynamic_slice_in_dim(butterfly_scale, at, local_cols, 0)
    pieces = lax.all_gather(piece, "row", axis=0)
    left = in_first_half("col")
    col_scale = jnp.where(left, pieces[0], pieces[row_count // 2]) * 0.5

    mixes, acrosses = [], []
    for j, (start, size, first, second) in enumerate(parts):
        mixes.append(mix_rows(slab_pair, theirs[j], start, first))
        acrosses.append(from_partner(mixes[j], second))

    out = unwritten(slab_pair.shape, slab_pair.dtype)
    for j in finish_order(len(parts)):
        start, _, _, axis = parts[j]
        out = finish_rows(out, mixes[j], acrosses[j], butterfly_scale, col_scale, start, axis)
    return out


def finish_order(n):
    return [j ^ 1 for j in range(n)]


def solution(mesh):
    in_specs = (P("row", "col"), P("row"))
    out_specs = P("row", "col")
    return jax.shard_map(
        per_device, mesh=mesh, in_specs=in_specs, out_specs=out_specs, check_vma=False
    )
```

```python
import jax
import jax.numpy as jnp
from jax import lax
from jax.experimental import pallas as pl
from jax.experimental.pallas import tpu as pltpu
from jax.sharding import PartitionSpec as P


N = 65536
W = 2048
SIZES = (512, 2688, 704, 192)


def from_partner(block, axis):
    count = lax.axis_size(axis)
    return lax.ppermute(block, axis, [(i, i ^ count // 2) for i in range(count)])


def in_first_half(axis):
    return lax.axis_index(axis) < lax.axis_size(axis) // 2


def kept_apart(*arrays):
    return lax.optimization_barrier(arrays)


def copy_rows(x, start, size):
    (x,) = kept_apart(x)
    return lax.slice_in_dim(x, start, start + size)


def copy_first(x, starts, size):
    pieces = 4
    step = size // pieces

    def kernel(x_ref, *refs):
        out_refs, sems = refs[:-1], refs[-1]
        copies = []
        for p in range(pieces):
            for k, (start, out_ref) in enumerate(zip(starts, out_refs)):
                copies.append(
                    pltpu.make_async_copy(
                        x_ref.at[pl.ds(start + p * step, step), :],
                        out_ref.at[pl.ds(p * step, step), :],
                        sems.at[k, p],
                    )
                )
        for copy in copies:
            copy.start()
        for copy in copies:
            copy.wait()

    return pl.pallas_call(
        kernel,
        in_specs=[pl.BlockSpec(memory_space=pltpu.HBM)],
        out_specs=[pl.BlockSpec(memory_space=pltpu.VMEM)] * len(starts),
        out_shape=[pltpu.VMEM((size, x.shape[1]), x.dtype)] * len(starts),
        scratch_shapes=[pltpu.SemaphoreType.DMA((len(starts), pieces))],
    )(x)


def mix_rows(x, partner, start, axis):
    x, partner = kept_apart(x, partner)
    block = lax.slice_in_dim(x, start, start + partner.shape[0])
    return jnp.where(in_first_half(axis), partner + block, partner - block)


def first_global_col(cols):
    first = lax.axis_index("col") * cols
    return jnp.where(first < W, first, N // 2 + first - W)


def unwritten(shape, dtype):
    return pl.pallas_call(
        lambda out_ref: None,
        out_specs=pl.BlockSpec(memory_space=pltpu.HBM),
        out_shape=jax.ShapeDtypeStruct(shape, dtype),
    )()


def factors(row_scale, col_scale, start, size):
    row_scale, col_scale = kept_apart(row_scale, col_scale)
    cols = col_scale.shape[0]
    gap = first_global_col(cols) - lax.axis_index("row") * row_scale.shape[0] - start
    row = lax.broadcasted_iota(jnp.int32, (size, cols), 0)
    col = lax.broadcasted_iota(jnp.int32, (size, cols), 1)
    scales = row_scale[start : start + size, None] * col_scale
    return jnp.where(row - col >= gap, scales, jnp.float32(0.0))


def finish_last(out, mixed, across, factor, start):
    size, cols = mixed.shape
    half = size // 2

    def kernel(mixed_ref, across_ref, factor_ref, _, out_ref, done_ref, sems):
        copies = []
        for p in range(2):
            rows = pl.ds(p * half, half)
            done_ref[rows, :] = (across_ref[rows, :] + mixed_ref[rows, :]) * factor_ref[rows, :]
            copy = pltpu.make_async_copy(
                done_ref.at[rows, :], out_ref.at[pl.ds(start + p * half, half), :], sems.at[p]
            )
            copy.start()
            copies.append(copy)
        for copy in copies:
            copy.wait()

    vmem = pl.BlockSpec(memory_space=pltpu.VMEM)
    hbm = pl.BlockSpec(memory_space=pltpu.HBM)
    held = [pltpu.with_memory_space_constraint(x, pltpu.VMEM) for x in (mixed, across, factor)]
    return pl.pallas_call(
        kernel,
        in_specs=[vmem, vmem, vmem, hbm],
        out_specs=hbm,
        out_shape=jax.ShapeDtypeStruct(out.shape, out.dtype),
        scratch_shapes=[pltpu.VMEM((size, cols), mixed.dtype), pltpu.SemaphoreType.DMA((2,))],
        input_output_aliases={3: 0},
    )(*held, out)


def finish_rows(out, mixed, across, row_scale, col_scale, start, axis):
    size, cols = mixed.shape
    both = jnp.where(in_first_half(axis), across + mixed, across - mixed)
    both = both * (row_scale[start : start + size, None] * col_scale)
    gap = first_global_col(cols) - lax.axis_index("row") * row_scale.shape[0] - start
    row = lax.broadcasted_iota(jnp.int32, (size, cols), 0)
    col = lax.broadcasted_iota(jnp.int32, (size, cols), 1)
    kept = jnp.where(row - col >= gap, both, jnp.float32(0.0))
    return lax.dynamic_update_slice(out, kept, (start, 0))


def per_device(slab_pair, butterfly_scale):
    local_rows, local_cols = slab_pair.shape
    row_count = lax.axis_size("row")
    parts = []
    start = 0
    for size in SIZES:
        parts.append((start, size, "row", "col"))
        parts.append((local_rows // 2 + start, size, "col", "row"))
        start += size

    theirs = []
    firsts = copy_first(slab_pair, [part[0] for part in parts[:2]], SIZES[0])
    for j, (start, size, first, _) in enumerate(parts):
        block = firsts[j] if j < 2 else copy_rows(slab_pair, start, size)
        theirs.append(from_partner(block, first))

    at = lax.axis_index("col") * local_cols % W
    piece = lax.dynamic_slice_in_dim(butterfly_scale, at, local_cols, 0)
    pieces = lax.all_gather(piece, "row", axis=0)
    left = in_first_half("col")
    col_scale = jnp.where(left, pieces[0], pieces[row_count // 2]) * 0.5

    mixes, acrosses = [], []
    for j, (start, size, first, second) in enumerate(parts):
        mixes.append(mix_rows(slab_pair, theirs[j], start, first))
        acrosses.append(from_partner(mixes[j], second))

    out = unwritten(slab_pair.shape, slab_pair.dtype)
    for j in finish_order(len(parts)):
        start, size, _, axis = parts[j]
        if j == len(parts) - 2:
            (mixed,) = kept_apart(mixes[j])
            mixed = jnp.where(in_first_half(axis), mixed, -mixed)
            factor = factors(butterfly_scale, col_scale, start, size)
            mixed, factor = kept_apart(mixed, factor)
            out = finish_last(out, mixed, acrosses[j], factor, start)
            continue
        out = finish_rows(out, mixes[j], acrosses[j], butterfly_scale, col_scale, start, axis)
    return out


def finish_order(n):
    return [j ^ 1 for j in range(n)]


def solution(mesh):
    in_specs = (P("row", "col"), P("row"))
    out_specs = P("row", "col")
    return jax.shard_map(
        per_device, mesh=mesh, in_specs=in_specs, out_specs=out_specs, check_vma=False
    )
```

```python
import jax
import jax.numpy as jnp
from jax import lax
from jax.experimental import pallas as pl
from jax.experimental.pallas import tpu as pltpu
from jax.sharding import PartitionSpec as P


N = 65536
W = 2048
SIZES = (512, 2752, 672, 160)
LAST = 2


def from_partner(block, axis):
    count = lax.axis_size(axis)
    return lax.ppermute(block, axis, [(i, i ^ count // 2) for i in range(count)])


def from_needed_partner(block, axis):
    if axis == "row":
        return from_partner(block, axis)
    rows, cols = lax.axis_size("row"), lax.axis_size("col")
    pairs = [
        (r * cols + c, r * cols + (c ^ cols // 2))
        for r in range(rows)
        for c in range(cols)
        if r >= rows // 2 or c >= cols // 2
    ]
    return lax.ppermute(block, ("row", "col"), pairs)


def in_first_half(axis):
    return lax.axis_index(axis) < lax.axis_size(axis) // 2


def kept_apart(*arrays):
    return lax.optimization_barrier(arrays)


def copy_rows(x, start, size):
    (x,) = kept_apart(x)
    return lax.slice_in_dim(x, start, start + size)


def copy_first(x, starts, size):
    pieces = 4
    step = size // pieces

    def kernel(x_ref, *refs):
        out_refs, sems = refs[:-1], refs[-1]
        copies = []
        for p in range(pieces):
            for k, (start, out_ref) in enumerate(zip(starts, out_refs)):
                copies.append(
                    pltpu.make_async_copy(
                        x_ref.at[pl.ds(start + p * step, step), :],
                        out_ref.at[pl.ds(p * step, step), :],
                        sems.at[k, p],
                    )
                )
        for copy in copies:
            copy.start()
        for copy in copies:
            copy.wait()

    return pl.pallas_call(
        kernel,
        in_specs=[pl.BlockSpec(memory_space=pltpu.HBM)],
        out_specs=[pl.BlockSpec(memory_space=pltpu.VMEM)] * len(starts),
        out_shape=[pltpu.VMEM((size, x.shape[1]), x.dtype)] * len(starts),
        scratch_shapes=[pltpu.SemaphoreType.DMA((len(starts), pieces))],
    )(x)


def mix_rows(x, partner, start, axis):
    x, partner = kept_apart(x, partner)
    block = lax.slice_in_dim(x, start, start + partner.shape[0])
    return jnp.where(in_first_half(axis), partner + block, partner - block)


def first_global_col(cols):
    first = lax.axis_index("col") * cols
    return jnp.where(first < W, first, N // 2 + first - W)


def unwritten(shape, dtype):
    return pl.pallas_call(
        lambda out_ref: None,
        out_specs=pl.BlockSpec(memory_space=pltpu.HBM),
        out_shape=jax.ShapeDtypeStruct(shape, dtype),
    )()


def factors(row_scale, col_scale, start, size):
    row_scale, col_scale = kept_apart(row_scale, col_scale)
    cols = col_scale.shape[0]
    gap = first_global_col(cols) - lax.axis_index("row") * row_scale.shape[0] - start
    row = lax.broadcasted_iota(jnp.int32, (size, cols), 0)
    col = lax.broadcasted_iota(jnp.int32, (size, cols), 1)
    scales = row_scale[start : start + size, None] * col_scale
    return jnp.where(row - col >= gap, scales, jnp.float32(0.0))


def finish_last(out, mixed, across, factor, start):
    size, cols = mixed.shape
    half = size // 2

    def kernel(mixed_ref, across_ref, factor_ref, _, out_ref, done_ref, sems):
        copies = []
        for p in range(2):
            rows = pl.ds(p * half, half)
            done_ref[rows, :] = (across_ref[rows, :] + mixed_ref[rows, :]) * factor_ref[rows, :]
            copy = pltpu.make_async_copy(
                done_ref.at[rows, :], out_ref.at[pl.ds(start + p * half, half), :], sems.at[p]
            )
            copy.start()
            copies.append(copy)
        for copy in copies:
            copy.wait()

    vmem = pl.BlockSpec(memory_space=pltpu.VMEM)
    hbm = pl.BlockSpec(memory_space=pltpu.HBM)
    held = [pltpu.with_memory_space_constraint(x, pltpu.VMEM) for x in (mixed, across, factor)]
    return pl.pallas_call(
        kernel,
        in_specs=[vmem, vmem, vmem, hbm],
        out_specs=hbm,
        out_shape=jax.ShapeDtypeStruct(out.shape, out.dtype),
        scratch_shapes=[pltpu.VMEM((size, cols), mixed.dtype), pltpu.SemaphoreType.DMA((2,))],
        input_output_aliases={3: 0},
    )(*held, out)


def finish_rows(out, mixed, across, row_scale, col_scale, start, axis):
    size, cols = mixed.shape
    both = jnp.where(in_first_half(axis), across + mixed, across - mixed)
    both = both * (row_scale[start : start + size, None] * col_scale)
    gap = first_global_col(cols) - lax.axis_index("row") * row_scale.shape[0] - start
    row = lax.broadcasted_iota(jnp.int32, (size, cols), 0)
    col = lax.broadcasted_iota(jnp.int32, (size, cols), 1)
    kept = jnp.where(row - col >= gap, both, jnp.float32(0.0))
    return lax.dynamic_update_slice(out, kept, (start, 0))


def per_device(slab_pair, butterfly_scale):
    local_rows, local_cols = slab_pair.shape
    row_count = lax.axis_size("row")
    parts = []
    start = 0
    for size in SIZES:
        parts.append((start, size, "row", "col"))
        parts.append((local_rows // 2 + start, size, "col", "row"))
        start += size

    theirs = []
    firsts = copy_first(slab_pair, [part[0] for part in parts[:2]], SIZES[0])
    for j, (start, size, first, _) in enumerate(parts):
        block = firsts[j] if j < 2 else copy_rows(slab_pair, start, size)
        theirs.append(from_partner(block, first))

    at = lax.axis_index("col") * local_cols % W
    piece = lax.dynamic_slice_in_dim(butterfly_scale, at, local_cols, 0)
    pieces = lax.all_gather(piece, "row", axis=0)
    left = in_first_half("col")
    col_scale = jnp.where(left, pieces[0], pieces[row_count // 2]) * 0.5

    mixes, acrosses = [], []
    for j, (start, size, first, second) in enumerate(parts):
        mixes.append(mix_rows(slab_pair, theirs[j], start, first))
        acrosses.append(from_needed_partner(mixes[j], second))

    out = unwritten(slab_pair.shape, slab_pair.dtype)
    for j in finish_order(len(parts)):
        start, size, _, axis = parts[j]
        if j >= len(parts) - LAST:
            (mixed,) = kept_apart(mixes[j])
            mixed = jnp.where(in_first_half(axis), mixed, -mixed)
            factor = factors(butterfly_scale, col_scale, start, size)
            mixed, factor = kept_apart(mixed, factor)
            out = finish_last(out, mixed, acrosses[j], factor, start)
            continue
        out = finish_rows(out, mixes[j], acrosses[j], butterfly_scale, col_scale, start, axis)
    return out


def finish_order(n):
    return [j ^ 1 for j in range(n)]


def solution(mesh):
    in_specs = (P("row", "col"), P("row"))
    out_specs = P("row", "col")
    return jax.shard_map(
        per_device, mesh=mesh, in_specs=in_specs, out_specs=out_specs, check_vma=False
    )
```

```python
import jax
import jax.numpy as jnp
from jax import lax
from jax.experimental import pallas as pl
from jax.experimental.pallas import tpu as pltpu
from jax.sharding import PartitionSpec as P


N = 65536
W = 2048
SIZES = (512, 2720, 640, 224)


def from_partner(block, axis):
    count = lax.axis_size(axis)
    return lax.ppermute(block, axis, [(i, i ^ count // 2) for i in range(count)])


def from_needed_partner(block, axis):
    if axis == "row":
        return from_partner(block, axis)
    rows, cols = lax.axis_size("row"), lax.axis_size("col")
    pairs = [
        (r * cols + c, r * cols + (c ^ cols // 2))
        for r in range(rows)
        for c in range(cols)
        if r >= rows // 2 or c >= cols // 2
    ]
    return lax.ppermute(block, ("row", "col"), pairs)


def in_first_half(axis):
    return lax.axis_index(axis) < lax.axis_size(axis) // 2


def kept_apart(*arrays):
    return lax.optimization_barrier(arrays)


def copy_rows(x, start, size):
    (x,) = kept_apart(x)
    return lax.slice_in_dim(x, start, start + size)


def copy_first(x, starts, size):
    pieces = 4
    step = size // pieces

    def kernel(x_ref, *refs):
        out_refs, sems = refs[:-1], refs[-1]
        copies = []
        for p in range(pieces):
            for k, (start, out_ref) in enumerate(zip(starts, out_refs)):
                copies.append(
                    pltpu.make_async_copy(
                        x_ref.at[pl.ds(start + p * step, step), :],
                        out_ref.at[pl.ds(p * step, step), :],
                        sems.at[k, p],
                    )
                )
        for copy in copies:
            copy.start()
        for copy in copies:
            copy.wait()

    return pl.pallas_call(
        kernel,
        in_specs=[pl.BlockSpec(memory_space=pltpu.HBM)],
        out_specs=[pl.BlockSpec(memory_space=pltpu.VMEM)] * len(starts),
        out_shape=[pltpu.VMEM((size, x.shape[1]), x.dtype)] * len(starts),
        scratch_shapes=[pltpu.SemaphoreType.DMA((len(starts), pieces))],
    )(x)


def mix_rows(x, partner, start, axis):
    x, partner = kept_apart(x, partner)
    block = lax.slice_in_dim(x, start, start + partner.shape[0])
    return jnp.where(in_first_half(axis), partner + block, partner - block)


def first_global_col(cols):
    first = lax.axis_index("col") * cols
    return jnp.where(first < W, first, N // 2 + first - W)


def unwritten(shape, dtype):
    return pl.pallas_call(
        lambda out_ref: None,
        out_specs=pl.BlockSpec(memory_space=pltpu.HBM),
        out_shape=jax.ShapeDtypeStruct(shape, dtype),
    )()


def factors(row_scale, col_scale, start, size):
    row_scale, col_scale = kept_apart(row_scale, col_scale)
    cols = col_scale.shape[0]
    gap = first_global_col(cols) - lax.axis_index("row") * row_scale.shape[0] - start
    row = lax.broadcasted_iota(jnp.int32, (size, cols), 0)
    col = lax.broadcasted_iota(jnp.int32, (size, cols), 1)
    scales = row_scale[start : start + size, None] * col_scale
    return jnp.where(row - col >= gap, scales, jnp.float32(0.0))


def finish_last(out, chunks):
    size, cols = chunks[0][0].shape
    half = size // 2

    def kernel(*refs):
        out_ref, done_ref, sems = refs[-3:]
        copies = []
        for k, (_, _, _, start) in enumerate(chunks):
            mixed_ref, across_ref, factor_ref = refs[3 * k : 3 * k + 3]
            for p in range(2):
                rows = pl.ds(p * half, half)
                done_ref[k, rows, :] = (across_ref[rows, :] + mixed_ref[rows, :]) * factor_ref[rows, :]
                copy = pltpu.make_async_copy(
                    done_ref.at[k, rows, :], out_ref.at[pl.ds(start + p * half, half), :], sems.at[k, p]
                )
                copy.start()
                copies.append(copy)
        for copy in copies:
            copy.wait()

    vmem = pl.BlockSpec(memory_space=pltpu.VMEM)
    hbm = pl.BlockSpec(memory_space=pltpu.HBM)
    held = [pltpu.with_memory_space_constraint(x, pltpu.VMEM) for chunk in chunks for x in chunk[:3]]
    return pl.pallas_call(
        kernel,
        in_specs=[vmem] * len(held) + [hbm],
        out_specs=hbm,
        out_shape=jax.ShapeDtypeStruct(out.shape, out.dtype),
        scratch_shapes=[
            pltpu.VMEM((len(chunks), size, cols), jnp.float32),
            pltpu.SemaphoreType.DMA((len(chunks), 2)),
        ],
        input_output_aliases={len(held): 0},
    )(*held, out)


def finish_rows(out, mixed, across, row_scale, col_scale, start, axis):
    size, cols = mixed.shape
    both = jnp.where(in_first_half(axis), across + mixed, across - mixed)
    both = both * (row_scale[start : start + size, None] * col_scale)
    gap = first_global_col(cols) - lax.axis_index("row") * row_scale.shape[0] - start
    row = lax.broadcasted_iota(jnp.int32, (size, cols), 0)
    col = lax.broadcasted_iota(jnp.int32, (size, cols), 1)
    kept = jnp.where(row - col >= gap, both, jnp.float32(0.0))
    return lax.dynamic_update_slice(out, kept, (start, 0))


def per_device(slab_pair, butterfly_scale):
    local_rows, local_cols = slab_pair.shape
    row_count = lax.axis_size("row")
    parts = []
    start = 0
    for size in SIZES:
        parts.append((start, size, "row", "col"))
        parts.append((local_rows // 2 + start, size, "col", "row"))
        start += size

    theirs = []
    firsts = copy_first(slab_pair, [part[0] for part in parts[:2]], SIZES[0])
    for j, (start, size, first, _) in enumerate(parts):
        block = firsts[j] if j < 2 else copy_rows(slab_pair, start, size)
        theirs.append(from_partner(block, first))

    at = lax.axis_index("col") * local_cols % W
    piece = lax.dynamic_slice_in_dim(butterfly_scale, at, local_cols, 0)
    pieces = lax.all_gather(piece, "row", axis=0)
    left = in_first_half("col")
    col_scale = jnp.where(left, pieces[0], pieces[row_count // 2]) * 0.5

    mixes, acrosses = [], []
    for j, (start, size, first, second) in enumerate(parts):
        mixes.append(mix_rows(slab_pair, theirs[j], start, first))
        acrosses.append(from_needed_partner(mixes[j], second))

    out = unwritten(slab_pair.shape, slab_pair.dtype)
    last = []
    for j in finish_order(len(parts)):
        start, size, _, axis = parts[j]
        if j >= len(parts) - 2:
            (mixed,) = kept_apart(mixes[j])
            mixed = jnp.where(in_first_half(axis), mixed, -mixed)
            factor = factors(butterfly_scale, col_scale, start, size)
            mixed, factor = kept_apart(mixed, factor)
            last.append((mixed, acrosses[j], factor, start))
            continue
        out = finish_rows(out, mixes[j], acrosses[j], butterfly_scale, col_scale, start, axis)
    return finish_last(out, last)


def finish_order(n):
    return [j ^ 1 for j in range(n)]


def solution(mesh):
    in_specs = (P("row", "col"), P("row"))
    out_specs = P("row", "col")
    return jax.shard_map(
        per_device, mesh=mesh, in_specs=in_specs, out_specs=out_specs, check_vma=False
    )
```

```python
import jax
import jax.numpy as jnp
from jax import lax
from jax.experimental import pallas as pl
from jax.experimental.pallas import tpu as pltpu
from jax.sharding import PartitionSpec as P


N = 65536
W = 2048
SIZES = (512, 2656, 608, 320)


def from_partner(block, axis):
    count = lax.axis_size(axis)
    return lax.ppermute(block, axis, [(i, i ^ count // 2) for i in range(count)])


def from_partner_by_core(block, first):
    rows, cols = lax.axis_size("row"), lax.axis_size("col")
    pairs = []
    for r in range(rows):
        for c in range(cols):
            along_rows = c % 2 == first
            partner = (r ^ rows // 2, c) if along_rows else (r, c ^ cols // 2)
            pairs.append((r * cols + c, partner[0] * cols + partner[1]))
    return lax.ppermute(block, ("row", "col"), pairs)


def from_needed_partner(block, axis):
    if axis == "row":
        return from_partner(block, axis)
    rows, cols = lax.axis_size("row"), lax.axis_size("col")
    pairs = [
        (r * cols + c, r * cols + (c ^ cols // 2))
        for r in range(rows)
        for c in range(cols)
        if r >= rows // 2 or c >= cols // 2
    ]
    return lax.ppermute(block, ("row", "col"), pairs)


def in_first_half(axis):
    return lax.axis_index(axis) < lax.axis_size(axis) // 2


def kept_apart(*arrays):
    return lax.optimization_barrier(arrays)


def copy_rows(x, start, size):
    (x,) = kept_apart(x)
    return lax.slice_in_dim(x, start, start + size)


def copy_first(x, starts, size, first):
    pieces = 4
    step = size // pieces

    def kernel(x_ref, out_ref, sems):
        start = jnp.where(lax.axis_index("col") % 2 == first, starts[0], starts[1])
        copies = [
            pltpu.make_async_copy(
                x_ref.at[pl.ds(pl.multiple_of(start + p * step, step), step), :],
                out_ref.at[pl.ds(p * step, step), :],
                sems.at[p],
            )
            for p in range(pieces)
        ]
        for copy in copies:
            copy.start()
        for copy in copies:
            copy.wait()

    return pl.pallas_call(
        kernel,
        in_specs=[pl.BlockSpec(memory_space=pltpu.HBM)],
        out_specs=pl.BlockSpec(memory_space=pltpu.VMEM),
        out_shape=pltpu.VMEM((size, x.shape[1]), x.dtype),
        scratch_shapes=[pltpu.SemaphoreType.DMA((pieces,))],
    )(x)


def mix_rows(x, partner, start, axis):
    x, partner = kept_apart(x, partner)
    block = lax.slice_in_dim(x, start, start + partner.shape[0])
    return jnp.where(in_first_half(axis), partner + block, partner - block)


def first_global_col(cols):
    first = lax.axis_index("col") * cols
    return jnp.where(first < W, first, N // 2 + first - W)


def unwritten(shape, dtype):
    return pl.pallas_call(
        lambda out_ref: None,
        out_specs=pl.BlockSpec(memory_space=pltpu.HBM),
        out_shape=jax.ShapeDtypeStruct(shape, dtype),
    )()


def factors(row_scale, col_scale, start, size):
    row_scale, col_scale = kept_apart(row_scale, col_scale)
    cols = col_scale.shape[0]
    gap = first_global_col(cols) - lax.axis_index("row") * row_scale.shape[0] - start
    row = lax.broadcasted_iota(jnp.int32, (size, cols), 0)
    col = lax.broadcasted_iota(jnp.int32, (size, cols), 1)
    scales = row_scale[start : start + size, None] * col_scale
    return jnp.where(row - col >= gap, scales, jnp.float32(0.0))


def finish_last(out, chunks):
    size, cols = chunks[0][0].shape
    half = size // 2

    def kernel(*refs):
        out_ref, done_ref, sems = refs[-3:]
        copies = []
        for k, (_, _, _, start) in enumerate(chunks):
            mixed_ref, across_ref, factor_ref = refs[3 * k : 3 * k + 3]
            for p in range(2):
                rows = pl.ds(p * half, half)
                done_ref[k, rows, :] = (across_ref[rows, :] + mixed_ref[rows, :]) * factor_ref[rows, :]
                copy = pltpu.make_async_copy(
                    done_ref.at[k, rows, :], out_ref.at[pl.ds(start + p * half, half), :], sems.at[k, p]
                )
                copy.start()
                copies.append(copy)
        for copy in copies:
            copy.wait()

    vmem = pl.BlockSpec(memory_space=pltpu.VMEM)
    hbm = pl.BlockSpec(memory_space=pltpu.HBM)
    held = [pltpu.with_memory_space_constraint(x, pltpu.VMEM) for chunk in chunks for x in chunk[:3]]
    return pl.pallas_call(
        kernel,
        in_specs=[vmem] * len(held) + [hbm],
        out_specs=hbm,
        out_shape=jax.ShapeDtypeStruct(out.shape, out.dtype),
        scratch_shapes=[
            pltpu.VMEM((len(chunks), size, cols), jnp.float32),
            pltpu.SemaphoreType.DMA((len(chunks), 2)),
        ],
        input_output_aliases={len(held): 0},
    )(*held, out)


def finish_rows(out, mixed, across, row_scale, col_scale, start, axis):
    size, cols = mixed.shape
    both = jnp.where(in_first_half(axis), across + mixed, across - mixed)
    both = both * (row_scale[start : start + size, None] * col_scale)
    gap = first_global_col(cols) - lax.axis_index("row") * row_scale.shape[0] - start
    row = lax.broadcasted_iota(jnp.int32, (size, cols), 0)
    col = lax.broadcasted_iota(jnp.int32, (size, cols), 1)
    kept = jnp.where(row - col >= gap, both, jnp.float32(0.0))
    return lax.dynamic_update_slice(out, kept, (start, 0))


def per_device(slab_pair, butterfly_scale):
    local_rows, local_cols = slab_pair.shape
    row_count = lax.axis_size("row")
    parts = []
    start = 0
    for size in SIZES:
        parts.append((start, size, "row", "col"))
        parts.append((local_rows // 2 + start, size, "col", "row"))
        start += size

    first_starts = [part[0] for part in parts[:2]]
    got = []
    for j in range(2):
        block = copy_first(slab_pair, first_starts, SIZES[0], j)
        got.append(from_partner_by_core(block, j))
    core = lax.axis_index("col") % 2
    theirs = [jnp.where(core == j, got[0], got[1]) for j in range(2)]
    for j, (start, size, first, _) in enumerate(parts[2:], 2):
        block = copy_rows(slab_pair, start, size)
        theirs.append(from_partner(block, first))

    at = lax.axis_index("col") * local_cols % W
    piece = lax.dynamic_slice_in_dim(butterfly_scale, at, local_cols, 0)
    pieces = lax.all_gather(piece, "row", axis=0)
    left = in_first_half("col")
    col_scale = jnp.where(left, pieces[0], pieces[row_count // 2]) * 0.5

    mixes, acrosses = [], []
    for j, (start, size, first, second) in enumerate(parts):
        mixes.append(mix_rows(slab_pair, theirs[j], start, first))
        acrosses.append(from_needed_partner(mixes[j], second))

    out = unwritten(slab_pair.shape, slab_pair.dtype)
    last = []
    for j in finish_order(len(parts)):
        start, size, _, axis = parts[j]
        if j >= len(parts) - 2:
            (mixed,) = kept_apart(mixes[j])
            mixed = jnp.where(in_first_half(axis), mixed, -mixed)
            factor = factors(butterfly_scale, col_scale, start, size)
            mixed, factor = kept_apart(mixed, factor)
            last.append((mixed, acrosses[j], factor, start))
            continue
        out = finish_rows(out, mixes[j], acrosses[j], butterfly_scale, col_scale, start, axis)
    return finish_last(out, last)


def finish_order(n):
    return [j ^ 1 for j in range(n)]


def solution(mesh):
    in_specs = (P("row", "col"), P("row"))
    out_specs = P("row", "col")
    return jax.shard_map(
        per_device, mesh=mesh, in_specs=in_specs, out_specs=out_specs, check_vma=False
    )
```

```python
import jax
import jax.numpy as jnp
from jax import lax
from jax.experimental import pallas as pl
from jax.experimental.pallas import tpu as pltpu
from jax.sharding import PartitionSpec as P


N = 65536
W = 2048
SIZES = (512, 2656, 608, 320)


def from_partner(block, axis):
    count = lax.axis_size(axis)
    return lax.ppermute(block, axis, [(i, i ^ count // 2) for i in range(count)])


def from_partner_by_core(block, first):
    rows, cols = lax.axis_size("row"), lax.axis_size("col")
    pairs = []
    for r in range(rows):
        for c in range(cols):
            along_rows = c % 2 == first
            partner = (r ^ rows // 2, c) if along_rows else (r, c ^ cols // 2)
            pairs.append((r * cols + c, partner[0] * cols + partner[1]))
    return lax.ppermute(block, ("row", "col"), pairs)


def in_first_half(axis):
    return lax.axis_index(axis) < lax.axis_size(axis) // 2


def kept_apart(*arrays):
    return lax.optimization_barrier(arrays)


def copy_rows(x, start, size):
    (x,) = kept_apart(x)
    return lax.slice_in_dim(x, start, start + size)


def copy_first(x, starts, size, first):
    pieces = 4
    step = size // pieces

    def kernel(x_ref, out_ref, sems):
        start = jnp.where(lax.axis_index("col") % 2 == first, starts[0], starts[1])
        copies = [
            pltpu.make_async_copy(
                x_ref.at[pl.ds(pl.multiple_of(start + p * step, step), step), :],
                out_ref.at[pl.ds(p * step, step), :],
                sems.at[p],
            )
            for p in range(pieces)
        ]
        for copy in copies:
            copy.start()
        for copy in copies:
            copy.wait()

    return pl.pallas_call(
        kernel,
        in_specs=[pl.BlockSpec(memory_space=pltpu.HBM)],
        out_specs=pl.BlockSpec(memory_space=pltpu.VMEM),
        out_shape=pltpu.VMEM((size, x.shape[1]), x.dtype),
        scratch_shapes=[pltpu.SemaphoreType.DMA((pieces,))],
    )(x)


def mix_rows(x, partner, start, axis):
    x, partner = kept_apart(x, partner)
    block = lax.slice_in_dim(x, start, start + partner.shape[0])
    return jnp.where(in_first_half(axis), partner + block, partner - block)


def first_global_col(cols):
    first = lax.axis_index("col") * cols
    return jnp.where(first < W, first, N // 2 + first - W)


def unwritten(shape, dtype):
    return pl.pallas_call(
        lambda out_ref: None,
        out_specs=pl.BlockSpec(memory_space=pltpu.HBM),
        out_shape=jax.ShapeDtypeStruct(shape, dtype),
    )()


def factors(row_scale, col_scale, start, size):
    row_scale, col_scale = kept_apart(row_scale, col_scale)
    cols = col_scale.shape[0]
    gap = first_global_col(cols) - lax.axis_index("row") * row_scale.shape[0] - start
    row = lax.broadcasted_iota(jnp.int32, (size, cols), 0)
    col = lax.broadcasted_iota(jnp.int32, (size, cols), 1)
    scales = row_scale[start : start + size, None] * col_scale
    return jnp.where(row - col >= gap, scales, jnp.float32(0.0))


def finish_last(out, chunks):
    size, cols = chunks[0][0].shape
    half = size // 2

    def kernel(*refs):
        out_ref, done_ref, sems = refs[-3:]
        copies = []
        for k, (_, _, _, start) in enumerate(chunks):
            mixed_ref, across_ref, factor_ref = refs[3 * k : 3 * k + 3]
            for p in range(2):
                rows = pl.ds(p * half, half)
                done_ref[k, rows, :] = (across_ref[rows, :] + mixed_ref[rows, :]) * factor_ref[rows, :]
                copy = pltpu.make_async_copy(
                    done_ref.at[k, rows, :], out_ref.at[pl.ds(start + p * half, half), :], sems.at[k, p]
                )
                copy.start()
                copies.append(copy)
        for copy in copies:
            copy.wait()

    vmem = pl.BlockSpec(memory_space=pltpu.VMEM)
    hbm = pl.BlockSpec(memory_space=pltpu.HBM)
    held = [pltpu.with_memory_space_constraint(x, pltpu.VMEM) for chunk in chunks for x in chunk[:3]]
    return pl.pallas_call(
        kernel,
        in_specs=[vmem] * len(held) + [hbm],
        out_specs=hbm,
        out_shape=jax.ShapeDtypeStruct(out.shape, out.dtype),
        scratch_shapes=[
            pltpu.VMEM((len(chunks), size, cols), jnp.float32),
            pltpu.SemaphoreType.DMA((len(chunks), 2)),
        ],
        input_output_aliases={len(held): 0},
    )(*held, out)


def finish_rows(out, mixed, across, row_scale, col_scale, start, axis):
    size, cols = mixed.shape
    both = jnp.where(in_first_half(axis), across + mixed, across - mixed)
    both = both * (row_scale[start : start + size, None] * col_scale)
    gap = first_global_col(cols) - lax.axis_index("row") * row_scale.shape[0] - start
    row = lax.broadcasted_iota(jnp.int32, (size, cols), 0)
    col = lax.broadcasted_iota(jnp.int32, (size, cols), 1)
    kept = jnp.where(row - col >= gap, both, jnp.float32(0.0))
    return lax.dynamic_update_slice(out, kept, (start, 0))


def per_device(slab_pair, butterfly_scale):
    local_rows, local_cols = slab_pair.shape
    row_count = lax.axis_size("row")
    parts = []
    start = 0
    for size in SIZES:
        parts.append((start, size, "row", "col"))
        parts.append((local_rows // 2 + start, size, "col", "row"))
        start += size

    first_starts = [part[0] for part in parts[:2]]
    got = []
    for j in range(2):
        block = copy_first(slab_pair, first_starts, SIZES[0], j)
        got.append(from_partner_by_core(block, j))
    core = lax.axis_index("col") % 2
    theirs = [jnp.where(core == j, got[0], got[1]) for j in range(2)]
    for j, (start, size, first, _) in enumerate(parts[2:], 2):
        block = copy_rows(slab_pair, start, size)
        theirs.append(from_partner(block, first))

    at = lax.axis_index("col") * local_cols % W
    piece = lax.dynamic_slice_in_dim(butterfly_scale, at, local_cols, 0)
    pieces = lax.all_gather(piece, "row", axis=0)
    left = in_first_half("col")
    col_scale = jnp.where(left, pieces[0], pieces[row_count // 2]) * 0.5

    mixes, acrosses = [], []
    for j, (start, size, first, second) in enumerate(parts):
        mixes.append(mix_rows(slab_pair, theirs[j], start, first))
        acrosses.append(from_partner(mixes[j], second))

    out = unwritten(slab_pair.shape, slab_pair.dtype)
    last = []
    for j in finish_order(len(parts)):
        start, size, _, axis = parts[j]
        if j >= len(parts) - 2:
            (mixed,) = kept_apart(mixes[j])
            mixed = jnp.where(in_first_half(axis), mixed, -mixed)
            factor = factors(butterfly_scale, col_scale, start, size)
            mixed, factor = kept_apart(mixed, factor)
            last.append((mixed, acrosses[j], factor, start))
            continue
        out = finish_rows(out, mixes[j], acrosses[j], butterfly_scale, col_scale, start, axis)
    return finish_last(out, last)


def finish_order(n):
    return [j ^ 1 for j in range(n)]


def solution(mesh):
    in_specs = (P("row", "col"), P("row"))
    out_specs = P("row", "col")
    return jax.shard_map(
        per_device, mesh=mesh, in_specs=in_specs, out_specs=out_specs, check_vma=False
    )
```

```python
import jax
import jax.numpy as jnp
from jax import lax
from jax.experimental import pallas as pl
from jax.experimental.pallas import tpu as pltpu
from jax.sharding import PartitionSpec as P


N = 65536
W = 2048
SIZES = (512, 2848, 480, 256)
PIECES = 4


def from_partner(block, axis):
    count = lax.axis_size(axis)
    return lax.ppermute(block, axis, [(i, i ^ count // 2) for i in range(count)])


def from_partner_by_core(block, first):
    rows, cols = lax.axis_size("row"), lax.axis_size("col")
    pairs = []
    for r in range(rows):
        for c in range(cols):
            along_rows = c % 2 == first
            partner = (r ^ rows // 2, c) if along_rows else (r, c ^ cols // 2)
            pairs.append((r * cols + c, partner[0] * cols + partner[1]))
    return lax.ppermute(block, ("row", "col"), pairs)


def in_first_half(axis):
    return lax.axis_index(axis) < lax.axis_size(axis) // 2


def kept_apart(*arrays):
    return lax.optimization_barrier(arrays)


def copy_rows(x, start, size):
    (x,) = kept_apart(x)
    return lax.slice_in_dim(x, start, start + size)


def copy_first(x, starts, size, first):
    pieces = 4
    step = size // pieces

    def kernel(x_ref, out_ref, sems):
        start = jnp.where(lax.axis_index("col") % 2 == first, starts[0], starts[1])
        copies = [
            pltpu.make_async_copy(
                x_ref.at[pl.ds(pl.multiple_of(start + p * step, step), step), :],
                out_ref.at[pl.ds(p * step, step), :],
                sems.at[p],
            )
            for p in range(pieces)
        ]
        for copy in copies:
            copy.start()
        for copy in copies:
            copy.wait()

    return pl.pallas_call(
        kernel,
        in_specs=[pl.BlockSpec(memory_space=pltpu.HBM)],
        out_specs=pl.BlockSpec(memory_space=pltpu.VMEM),
        out_shape=pltpu.VMEM((size, x.shape[1]), x.dtype),
        scratch_shapes=[pltpu.SemaphoreType.DMA((pieces,))],
    )(x)


def mix_rows(x, partner, start, axis):
    x, partner = kept_apart(x, partner)
    block = lax.slice_in_dim(x, start, start + partner.shape[0])
    return jnp.where(in_first_half(axis), partner + block, partner - block)


def first_global_col(cols):
    first = lax.axis_index("col") * cols
    return jnp.where(first < W, first, N // 2 + first - W)


def unwritten(shape, dtype):
    return pl.pallas_call(
        lambda out_ref: None,
        out_specs=pl.BlockSpec(memory_space=pltpu.HBM),
        out_shape=jax.ShapeDtypeStruct(shape, dtype),
    )()


def factors(row_scale, col_scale, start, size):
    row_scale, col_scale = kept_apart(row_scale, col_scale)
    cols = col_scale.shape[0]
    gap = first_global_col(cols) - lax.axis_index("row") * row_scale.shape[0] - start
    row = lax.broadcasted_iota(jnp.int32, (size, cols), 0)
    col = lax.broadcasted_iota(jnp.int32, (size, cols), 1)
    scales = row_scale[start : start + size, None] * col_scale
    return jnp.where(row - col >= gap, scales, jnp.float32(0.0))


def finish_last(out, chunks):
    size, cols = chunks[0][0].shape
    piece = size // PIECES

    def kernel(*refs):
        out_ref, done_ref, sems = refs[-3:]
        copies = []
        for k, (_, _, _, start) in enumerate(chunks):
            mixed_ref, across_ref, factor_ref = refs[3 * k : 3 * k + 3]
            for p in range(PIECES):
                rows = pl.ds(p * piece, piece)
                done_ref[k, rows, :] = (across_ref[rows, :] + mixed_ref[rows, :]) * factor_ref[rows, :]
                copy = pltpu.make_async_copy(
                    done_ref.at[k, rows, :], out_ref.at[pl.ds(start + p * piece, piece), :], sems.at[k, p]
                )
                copy.start()
                copies.append(copy)
        for copy in copies:
            copy.wait()

    vmem = pl.BlockSpec(memory_space=pltpu.VMEM)
    hbm = pl.BlockSpec(memory_space=pltpu.HBM)
    held = [pltpu.with_memory_space_constraint(x, pltpu.VMEM) for chunk in chunks for x in chunk[:3]]
    return pl.pallas_call(
        kernel,
        in_specs=[vmem] * len(held) + [hbm],
        out_specs=hbm,
        out_shape=jax.ShapeDtypeStruct(out.shape, out.dtype),
        scratch_shapes=[
            pltpu.VMEM((len(chunks), size, cols), jnp.float32),
            pltpu.SemaphoreType.DMA((len(chunks), PIECES)),
        ],
        input_output_aliases={len(held): 0},
    )(*held, out)


def finish_rows(out, mixed, across, row_scale, col_scale, start, axis):
    size, cols = mixed.shape
    both = jnp.where(in_first_half(axis), across + mixed, across - mixed)
    both = both * (row_scale[start : start + size, None] * col_scale)
    gap = first_global_col(cols) - lax.axis_index("row") * row_scale.shape[0] - start
    row = lax.broadcasted_iota(jnp.int32, (size, cols), 0)
    col = lax.broadcasted_iota(jnp.int32, (size, cols), 1)
    kept = jnp.where(row - col >= gap, both, jnp.float32(0.0))
    return lax.dynamic_update_slice(out, kept, (start, 0))


def per_device(slab_pair, butterfly_scale):
    local_rows, local_cols = slab_pair.shape
    row_count = lax.axis_size("row")
    parts = []
    start = 0
    for size in SIZES:
        parts.append((start, size, "row", "col"))
        parts.append((local_rows // 2 + start, size, "col", "row"))
        start += size

    first_starts = [part[0] for part in parts[:2]]
    got = []
    for j in range(2):
        block = copy_first(slab_pair, first_starts, SIZES[0], j)
        got.append(from_partner_by_core(block, j))
    core = lax.axis_index("col") % 2
    theirs = [jnp.where(core == j, got[0], got[1]) for j in range(2)]
    for j, (start, size, first, _) in enumerate(parts[2:], 2):
        block = copy_rows(slab_pair, start, size)
        theirs.append(from_partner(block, first))

    at = lax.axis_index("col") * local_cols % W
    piece = lax.dynamic_slice_in_dim(butterfly_scale, at, local_cols, 0)
    pieces = lax.all_gather(piece, "row", axis=0)
    left = in_first_half("col")
    col_scale = jnp.where(left, pieces[0], pieces[row_count // 2]) * 0.5

    mixes, acrosses = [], []
    for j, (start, size, first, second) in enumerate(parts):
        mixes.append(mix_rows(slab_pair, theirs[j], start, first))
        acrosses.append(from_partner(mixes[j], second))

    out = unwritten(slab_pair.shape, slab_pair.dtype)
    last = []
    for j in finish_order(len(parts)):
        start, size, _, axis = parts[j]
        if j >= len(parts) - 2:
            (mixed,) = kept_apart(mixes[j])
            mixed = jnp.where(in_first_half(axis), mixed, -mixed)
            factor = factors(butterfly_scale, col_scale, start, size)
            mixed, factor = kept_apart(mixed, factor)
            last.append((mixed, acrosses[j], factor, start))
            continue
        out = finish_rows(out, mixes[j], acrosses[j], butterfly_scale, col_scale, start, axis)
    return finish_last(out, last)


def finish_order(n):
    return [j ^ 1 for j in range(n)]


def solution(mesh):
    in_specs = (P("row", "col"), P("row"))
    out_specs = P("row", "col")
    return jax.shard_map(
        per_device, mesh=mesh, in_specs=in_specs, out_specs=out_specs, check_vma=False
    )
```
